32 devices in a mesh: atoms: 8 (over y, x, core), gsplit: 4 (over z).
Axes of the slice: x: 2, y: 2, z: 4, core: 2. Of those that a mesh axis runs over, the one named last changes fastest.
Arguments:
- miller: int32 [3, 30720], P(None, 'gsplit'), may hold values from -16 to 16, as said below
- form_factors: bfloat16 [49, 30720], P(None, 'gsplit'), may hold values from -6 to 6
- fractional: float32 [3, 512], P(None, 'atoms'), may hold values from 0 to 1
- multipoles: bfloat16 [2, 49, 512], P(None, None, 'atoms'), may hold values from -0.0390625 to 0.0390625
- point_owner: int32 [1024], P(('atoms', 'gsplit')), may hold values from 0 to 63
- offsets: float32 [3, 1024], P(None, ('atoms', 'gsplit')), may hold values from -0.05 to 0.05
Outputs:
- grid_potential: float32 [2, 1024], P(None, ('atoms', 'gsplit'))
- moments: float32 [2, 49, 512], P(None, None, ('atoms', 'gsplit'))
The draws below stay inside these ranges and needn't reach their ends.
Inputs may be any that keep to these rules, and one draw needn't show every extreme that they name: `miller`: no vector has all three indices zero. Point p belongs to atom (p // 128) * 64 + point_owner[p].
All inputs are finite; a program needn't handle non-finite values.
Results may differ from the reference program's by a relative error of at most 0.0045.
Values may be sent and summed in bfloat16 or wider, within the bound.
A program may use at most 64 MiB of HBM per device.

```python
import math
import jax
import jax.numpy as jnp
from jax import lax

COMPS = 49
NG = 30720
DENS = 2
ATOM_BLK = 64
ATOMS = 512
P_BLK = 128
POINTS = 1024


def draw_miller(key, part):
    values = jax.random.randint(jax.random.fold_in(key, 11), (3, NG), -16, 17, dtype=jnp.int32)
    all_zero = jnp.all(values == 0, axis=0)
    first_row = jnp.where(all_zero, 1, values[0]).astype(jnp.int32)
    return jnp.concatenate([first_row[None, :], values[1:]], axis=0).astype(jnp.int32)


def set_ends(values, key, least, high):
    longest = values.shape.index(max(values.shape))
    spots = []
    for shift in (0, 1):
        where = [jax.random.randint(jax.random.fold_in(key, axis), (), 0, length) for axis, length in enumerate(values.shape)]
        where[longest] = (where[longest] + shift) % values.shape[longest]
        spots.append(tuple(where))
    return values.at[spots[0]].set(least).at[spots[1]].set(high)


def shard_levels(rng, dims, cuts, smallest, high):
    factor_of, own = 1.0, jax.random.fold_in(rng, 6)
    for dim, parts in cuts:
        steps = jnp.exp(jax.random.uniform(jax.random.fold_in(own, dim), (parts,), jnp.float32, smallest / len(cuts), high / len(cuts)))
        factor_of = factor_of * jnp.repeat(steps, dims[dim] // parts).reshape([-1 if axis == dim else 1 for axis in range(len(dims))])
    return factor_of


def normal_values(key, dims, scale, bound, split=(), kind=jnp.bfloat16):
    drawn = jax.random.normal(key, dims, jnp.float32) * scale
    if len(split) > 0:
        drawn = shard_levels(key, dims, split, -0.22, 0.18) * drawn
    return jnp.clip(drawn, min=-bound, max=bound).astype(kind)


def setup_inputs(seed: int = 0) -> dict:
    keys = jax.random.split(jax.random.key(seed), 7)
    miller = draw_miller(jax.random.fold_in(keys[6], 71), 0)
    form_factors = normal_values(keys[1], (COMPS, NG), 1.0, 6.0, ((1, 4),))
    fractional = jnp.clip(1.0 * jax.random.uniform(keys[2], (3, ATOMS), jnp.float32) ** shard_levels(keys[2], (3, ATOMS), ((1, 8),), -0.2, 0.2), 0.0, 1.0)
    multipoles = normal_values(keys[3], (DENS, COMPS, ATOMS), (ATOMS * COMPS) ** -0.5, 0.0390625, ((2, 8),))
    point_owner = set_ends(jax.random.randint(keys[4], (POINTS,), 0, ATOM_BLK), jax.random.fold_in(keys[4], 1), 0, ATOM_BLK - 1).astype(jnp.int32)
    offsets = jnp.clip(jax.random.uniform(keys[5], (3, POINTS), jnp.float32, -0.05, 0.05) * shard_levels(keys[5], (3, POINTS), ((1, 32),), -0.4, 0.0), -0.05, 0.05)
    return dict(miller=miller, form_factors=form_factors, fractional=fractional, multipoles=multipoles, point_owner=point_owner, offsets=offsets)


two_pi = 2.0 * math.pi
damping = 1.0 / 400.0


def angles(vectors, places):
    indices = vectors.astype(jnp.float32)
    summed = places[0][:, None] * indices[0][None, :] + places[1][:, None] * indices[1][None, :] + places[2][:, None] * indices[2][None, :]
    return two_pi * summed


def sign_tables(comp_count):
    comp_ids = jnp.arange(comp_count, dtype=jnp.int32)
    degree = jnp.zeros((comp_count,), jnp.int32)
    for degree_step in range(1, 16):
        degree = degree + (comp_ids >= degree_step * degree_step).astype(jnp.int32)
    quarter = degree % 4
    even_sign = jnp.where(quarter == 0, 1.0, jnp.where(quarter == 2, -1.0, 0.0)).astype(jnp.float32)
    odd_sign = jnp.where(quarter == 3, 1.0, jnp.where(quarter == 1, -1.0, 0.0)).astype(jnp.float32)
    return even_sign, odd_sign


def coulomb(vectors):
    indices = vectors.astype(jnp.float32)
    square = indices[0] * indices[0] + indices[1] * indices[1] + indices[2] * indices[2]
    return jnp.exp(-damping * square) / square


def structure(multipoles, cos_table, sin_table, form_block, even_sign, odd_sign):
    density_count, comp_count, atom_count = multipoles.shape
    flattened = multipoles.reshape(density_count * comp_count, atom_count)
    along_cos = jnp.dot(flattened, cos_table, preferred_element_type=jnp.float32).reshape(density_count, comp_count, -1)
    along_sin = jnp.dot(flattened, sin_table, preferred_element_type=jnp.float32).reshape(density_count, comp_count, -1)
    weights = form_block.astype(jnp.float32)[None]
    even_wide = even_sign[None, :, None]
    odd_wide = odd_sign[None, :, None]
    real_part = jnp.sum(weights * (even_wide * along_cos + odd_wide * along_sin), axis=1)
    imag_part = jnp.sum(weights * (odd_wide * along_cos - even_wide * along_sin), axis=1)
    return jnp.stack([real_part, imag_part], axis=1)


def moment_terms(potential, form_block, cos_table, sin_table, even_sign, odd_sign):
    weighted = (form_block.astype(jnp.float32)[None, None] * potential[:, :, None, :]).astype(jnp.bfloat16)
    density_count, _, comp_count, vector_count = weighted.shape
    flattened = weighted.reshape(density_count * 2 * comp_count, vector_count)
    contract = (((1,), (1,)), ((), ()))
    with_cos = lax.dot_general(flattened, cos_table, contract, preferred_element_type=jnp.float32).reshape(density_count, 2, comp_count, -1)
    with_sin = lax.dot_general(flattened, sin_table, contract, preferred_element_type=jnp.float32).reshape(density_count, 2, comp_count, -1)
    even_wide = even_sign[None, :, None]
    odd_wide = odd_sign[None, :, None]
    return even_wide * with_cos[:, 0] + odd_wide * with_sin[:, 0] + odd_wide * with_cos[:, 1] - even_wide * with_sin[:, 1]


def grid_rows(rounded, vectors, places):
    point_angles = angles(vectors, places)
    cos_points = jnp.cos(point_angles).astype(jnp.bfloat16)
    sin_points = jnp.sin(point_angles).astype(jnp.bfloat16)
    contract = (((1,), (1,)), ((), ()))
    return lax.dot_general(cos_points, rounded[:, 0], contract, preferred_element_type=jnp.float32) - lax.dot_general(sin_points, rounded[:, 1], contract, preferred_element_type=jnp.float32)


def reference(miller, form_factors, fractional, multipoles, point_owner, offsets):
    even_sign, odd_sign = sign_tables(COMPS)
    blocks = 32
    block_width = NG // blocks
    point_index = jnp.arange(POINTS, dtype=jnp.int32)
    owner_index = ((point_index // P_BLK) * ATOM_BLK + point_owner).astype(jnp.int32)
    places = jnp.take(fractional, owner_index, axis=1) + offsets
    vector_blocks = miller.reshape(3, blocks, block_width).transpose(1, 0, 2)
    form_blocks = form_factors.reshape(COMPS, blocks, block_width).transpose(1, 0, 2)

    def advance(carried, pieces):
        moment_sum, grid_sum = carried
        vectors, form_block = pieces
        phases = angles(vectors, fractional)
        cos_table = jnp.cos(phases).astype(jnp.bfloat16)
        sin_table = jnp.sin(phases).astype(jnp.bfloat16)
        summed = structure(multipoles, cos_table, sin_table, form_block, even_sign, odd_sign)
        potential = coulomb(vectors)[None, None, :] * summed
        moment_sum = moment_sum + moment_terms(potential, form_block, cos_table, sin_table, even_sign, odd_sign)
        grid_sum = grid_sum + grid_rows(potential.astype(jnp.bfloat16), vectors, places)
        return (moment_sum, grid_sum), None

    initial = (jnp.zeros((DENS, COMPS, ATOMS), jnp.float32), jnp.zeros((POINTS, DENS), jnp.float32))
    (moment_sum, grid_sum), _ = lax.scan(advance, initial, (vector_blocks, form_blocks))
    return grid_sum.T, moment_sum
```

```python
import functools

import jax
import jax.numpy as jnp
from jax import lax
from jax.experimental import pallas as pl
from jax.experimental.pallas import tpu as pltpu
from jax.sharding import PartitionSpec as P

damping = 1.0 / 400.0
MESH = pl.DeviceIdType.MESH
f32 = jnp.float32
bf16 = jnp.bfloat16

SIN_COEFS = (4.442879567546084, -7.30781668449178, 3.5977741780871235, -0.7911993921609659)
COS_COEFS = (
    1.4142134962552286,
    -6.978850948563789,
    5.73946037690675,
    -1.8835579059841712,
    0.3106880275217573,
)


def poly(coefs, x):
    total = coefs[-1]
    for coef in coefs[-2::-1]:
        total = total * x + coef
    return total


def cos_sin(turns):
    r = turns - jnp.round(turns)
    square = r * r
    half_sin = r * poly(SIN_COEFS, square)
    half_cos = poly(COS_COEFS, square)
    return (1.0 - half_sin * half_sin).astype(bf16), (half_sin * half_cos).astype(bf16)


def three_parts(x):
    first = x.astype(bf16).astype(f32)
    rest = x - first
    second = rest.astype(bf16).astype(f32)
    third = rest - second
    return jnp.concatenate([first, second, third, jnp.zeros_like(x)], axis=0)


def row_signs(comps, rows):
    ids = lax.broadcasted_iota(jnp.int32, (rows, 1), 0)
    degree = jnp.zeros_like(ids)
    for step in range(1, 16):
        if step * step < comps:
            degree = degree + (ids >= step * step).astype(jnp.int32)
    quarter = lax.rem(degree, 4)
    quarter = jnp.where(ids == comps, 0, quarter)
    even = (quarter == 0) | (quarter == 2)
    sign = jnp.where((quarter == 0) | (quarter == 3), 1.0, -1.0).astype(f32)
    return even, sign


def kernel(
    n_atoms, n_split, chunk,
    miller_ref, form_ref, frac_ref, mult_ref, owner_ref, offs_ref,
    grid_out, mom_out,
    vec8, fx, tcos, tsin, partial, from_core, acc, hop_in, total, place_buf, send_buf, recv_buf,
    core_sems, hop_send, hop_recv, back_sems, place_send, place_recv, out_send, out_recv,
):
    me = lax.axis_index("atoms")
    mine = lax.axis_index("gsplit")
    dens, comps, atoms = mult_ref.shape
    rows = fx.shape[0]
    width = partial.shape[3]
    steps = width // chunk
    points = n_split * owner_ref.shape[0]
    own_points = owner_ref.shape[0]
    bits = n_atoms.bit_length() - 1
    core = lax.rem(me, 2)
    other = 1 - core

    def flipped(bit):
        return me + (1 - 2 * lax.rem(lax.div(me, 2**bit), 2)) * 2**bit

    barrier = pltpu.get_barrier_semaphore()
    for bit in range(bits):
        pl.semaphore_signal(barrier, inc=1, device_id={"atoms": flipped(bit)}, device_id_type=MESH)
    for away in range(1, n_split):
        pl.semaphore_signal(
            barrier, inc=1, device_id={"gsplit": lax.rem(mine + away, n_split)}, device_id_type=MESH
        )

    even, sign = row_signs(comps, rows)

    vec8[...] = jnp.zeros_like(vec8)
    vec8[0:3, :] = miller_ref[...].astype(f32)

    tail = (comps // 8) * 8
    tail_ids = lax.broadcasted_iota(jnp.int32, (rows - tail, fx.shape[1]), 0)
    fx[tail:rows, :] = jnp.where(tail_ids == comps - tail, 1.0, 0.0).astype(f32)
    fx[0:comps, :] = form_ref[...].astype(f32) * sign[0:comps]

    frac8 = jnp.concatenate([frac_ref[...], jnp.zeros((5, atoms), f32)], axis=0)
    frac_parts = three_parts(frac8)
    atom_ids = lax.broadcasted_iota(jnp.int32, (atoms, own_points), 0)
    onehot = (atom_ids == owner_ref[...].reshape(1, own_points)).astype(f32).astype(bf16)
    picked = jnp.dot(frac_parts.astype(bf16), onehot, preferred_element_type=f32)
    place = (picked[0:8] + picked[8:16]) + picked[16:24]
    place_buf[mine, :, :] = jnp.zeros(place_buf.shape[1:], f32)
    place_buf[mine, :, 0:own_points] = place
    place_buf[mine, 0:3, 0:own_points] = place[0:3] + offs_ref[...]

    def widened(block):
        pad = jnp.zeros((block.shape[0], 128 - block.shape[1]), f32)
        return jnp.concatenate([block, pad], axis=1).T if pad.shape[1] else block.T

    atom_parts = widened(frac_parts)[0:atoms].astype(bf16)

    groups = []
    for part in range(2):
        for d in range(dens):
            m = jnp.concatenate(
                [mult_ref[d].astype(f32), jnp.zeros((rows - comps, atoms), f32)], axis=0
            )
            if part == 0:
                with_cos, with_sin = jnp.where(even, m, 0.0), jnp.where(even, 0.0, m)
            else:
                with_cos, with_sin = jnp.where(even, 0.0, m), jnp.where(even, -m, 0.0)
            groups.append(jnp.concatenate([with_cos, with_sin], axis=1))
    against = jnp.concatenate(groups, axis=0).astype(bf16)

    def vectors(half, quarter, i):
        start = pl.multiple_of(half * 2 * width + quarter * width + i * chunk, 128)
        return pl.ds(start, chunk)

    def turns(parts, where):
        v = vec8[:, where]
        wide = jnp.concatenate([v, v, v, jnp.zeros_like(v)], axis=0).astype(bf16)
        return jnp.dot(parts, wide, preferred_element_type=f32)

    def within(quarter, i):
        return pl.ds(pl.multiple_of(quarter * width + i * chunk, 128), chunk)

    def structure(half, quarter):
        def body(i, carry):
            where = vectors(half, quarter, i)
            inside = within(quarter, i)
            c, s = cos_sin(turns(atom_parts, where))
            tcos[half, 0:atoms, inside] = c
            tsin[half, 0:atoms, inside] = s
            both = jnp.concatenate([c, s], axis=0)
            along = jnp.dot(against, both, preferred_element_type=f32)
            f = fx[:, where]
            sums = [
                jnp.sum(f * along[k * rows : (k + 1) * rows], axis=0, keepdims=True)
                for k in range(2 * dens)
            ]
            lanes = pl.ds(pl.multiple_of(i * chunk, 128), chunk)
            partial[half, quarter, :, lanes] = jnp.concatenate(sums, axis=0)
            return carry

        lax.fori_loop(0, steps, body, 0)

    structure(other, 0)
    structure(other, 1)

    pl.semaphore_wait(barrier, bits + n_split - 1)

    place_copies = []
    for away in range(1, n_split):
        copy = pltpu.make_async_remote_copy(
            src_ref=place_buf.at[mine],
            dst_ref=place_buf.at[mine],
            send_sem=place_send.at[away],
            recv_sem=place_recv.at[away],
            device_id={"gsplit": lax.rem(mine + away, n_split)},
            device_id_type=MESH,
        )
        copy.start()
        place_copies.append(copy)
    to_core = pltpu.make_async_remote_copy(
        src_ref=partial.at[other],
        dst_ref=from_core,
        send_sem=core_sems.at[0],
        recv_sem=core_sems.at[1],
        device_id={"atoms": flipped(0)},
        device_id_type=MESH,
    )
    to_core.start()

    structure(core, 0)
    structure(core, 1)

    def hop(stage, quarter):
        bit = 1 + stage if quarter == 0 else bits - 1 - stage
        return pltpu.make_async_remote_copy(
            src_ref=acc.at[stage, quarter],
            dst_ref=hop_in.at[stage, quarter],
            send_sem=hop_send.at[stage, quarter],
            recv_sem=hop_recv.at[stage, quarter],
            device_id={"atoms": flipped(bit)},
            device_id_type=MESH,
        )

    to_core.wait()
    hops = {}
    for quarter in range(2):
        acc[0, quarter] = partial[core, quarter] + from_core[quarter]
        if bits > 1:
            hops[0, quarter] = hop(0, quarter)
            hops[0, quarter].start()

    for copy in place_copies:
        copy.wait()
    pieces = [three_parts(place_buf[k, :, 0:own_points]) for k in range(n_split)]
    point_parts = widened(jnp.concatenate(pieces, axis=1))[0:points].astype(bf16)

    def point_tables(half, quarter):
        def body(i, carry):
            inside = within(quarter, i)
            c, s = cos_sin(turns(point_parts, vectors(half, quarter, i)))
            tcos[half, atoms : atoms + points, inside] = c
            tsin[half, atoms : atoms + points, inside] = s
            return carry

        lax.fori_loop(0, steps, body, 0)

    work = [(h, q) for h in range(2) for q in range(2)]
    stages = bits - 1
    for stage in range(stages):
        share = work[stage * len(work) // stages : (stage + 1) * len(work) // stages]
        for half, quarter in share:
            point_tables(half, quarter)
        for quarter in range(2):
            hops[stage, quarter].wait()
            summed = acc[stage, quarter] + hop_in[stage, quarter]
            if stage + 1 < stages:
                acc[stage + 1, quarter] = summed
                hops[stage + 1, quarter] = hop(stage + 1, quarter)
                hops[stage + 1, quarter].start()
            else:
                total[core, quarter] = summed
    back = pltpu.make_async_remote_copy(
        src_ref=total.at[core],
        dst_ref=total.at[core],
        send_sem=back_sems.at[0],
        recv_sem=back_sems.at[1],
        device_id={"atoms": flipped(0)},
        device_id_type=MESH,
    )
    back.start()

    def moments(half):
        result = None
        for quarter in range(2):
            start = pl.multiple_of(half * 2 * width + quarter * width, 128)
            where = pl.ds(start, width)
            v = vec8[:, where]
            q = jnp.sum(v * v, axis=0, keepdims=True)
            pot = (jnp.exp(-damping * q) / q) * total[half, quarter]
            f = fx[:, where]
            lanes = slice(quarter * width, (quarter + 1) * width)
            with_cos, with_sin = [], []
            for d in range(dens):
                re, im = pot[d : d + 1], pot[dens + d : dens + d + 1]
                with_cos.append(f * jnp.where(even, re, im))
                with_sin.append(f * jnp.where(even, -im, re))
            for table, weights in ((tcos, with_cos), (tsin, with_sin)):
                term = lax.dot_general(
                    table[half, :, lanes],
                    jnp.concatenate(weights, axis=0).astype(bf16),
                    (((1,), (1,)), ((), ())),
                    preferred_element_type=f32,
                )
                result = term if result is None else result + term
        return result

    own = moments(core)
    back.wait()
    local = own + moments(other)

    pad = jnp.zeros((local.shape[0], 128 - local.shape[1]), f32)
    local = jnp.concatenate([local, pad], axis=1)
    grid_rows = local[atoms : atoms + points].T
    share = atoms // n_split
    for k in range(n_split):
        send_buf[k, 0:share, :] = local[k * share : (k + 1) * share]
        send_buf[k, share:, :] = jnp.zeros((8, 128), f32)
        for d in range(dens):
            row = d * rows + comps
            send_buf[k, share + d : share + d + 1, 0:own_points] = grid_rows[
                row : row + 1, k * own_points : (k + 1) * own_points
            ]
    out_copies = []
    for away in range(1, n_split):
        there = lax.rem(mine + away, n_split)
        copy = pltpu.make_async_remote_copy(
            src_ref=send_buf.at[there],
            dst_ref=recv_buf.at[away],
            send_sem=out_send.at[away],
            recv_sem=out_recv.at[away],
            device_id={"gsplit": there},
            device_id_type=MESH,
        )
        copy.start()
        out_copies.append(copy)
    result = send_buf[mine]
    for away, copy in enumerate(out_copies, 1):
        copy.wait()
        result = result + recv_buf[away]
    grid_out[...] = result[share : share + dens, 0:own_points]
    if share < 128:
        square = jnp.concatenate([result[0:share], jnp.zeros((128 - share, 128), f32)], axis=0)
    by_comp = square.T
    for d in range(dens):
        mom_out[d] = by_comp[d * rows : d * rows + comps, 0:share]


def shards(n_atoms, n_split, miller, form_factors, fractional, multipoles, point_owner, offsets):
    dens, comps, atoms = multipoles.shape
    vectors = miller.shape[1]
    width = vectors // 4
    chunk = max(c for c in (128, 256, 384) if width % c == 0)
    rows = (comps + 1 + 7) // 8 * 8
    own_points = point_owner.shape[0]
    table_rows = atoms + n_split * own_points
    stages = max(n_atoms.bit_length() - 2, 1)
    share = atoms // n_split
    vmem = pl.BlockSpec(memory_space=pltpu.VMEM)
    dma = pltpu.SemaphoreType.DMA
    return pl.pallas_call(
        functools.partial(kernel, n_atoms, n_split, chunk),
        out_shape=(
            jax.ShapeDtypeStruct((dens, own_points), f32),
            jax.ShapeDtypeStruct((dens, comps, share), f32),
        ),
        in_specs=[vmem] * 6,
        out_specs=(vmem, vmem),
        scratch_shapes=[
            pltpu.VMEM((8, vectors), f32),
            pltpu.VMEM((rows, vectors), f32),
            pltpu.VMEM((2, table_rows, 2 * width), bf16),
            pltpu.VMEM((2, table_rows, 2 * width), bf16),
            pltpu.VMEM((2, 2, 2 * dens, width), f32),
            pltpu.VMEM((2, 2 * dens, width), f32),
            pltpu.VMEM((stages, 2, 2 * dens, width), f32),
            pltpu.VMEM((stages, 2, 2 * dens, width), f32),
            pltpu.VMEM((2, 2, 2 * dens, width), f32),
            pltpu.VMEM((n_split, 8, 128), f32),
            pltpu.VMEM((n_split, share + 8, 128), f32),
            pltpu.VMEM((n_split, share + 8, 128), f32),
            dma((2,)),
            dma((stages, 2)),
            dma((stages, 2)),
            dma((2,)),
            dma((n_split,)),
            dma((n_split,)),
            dma((n_split,)),
            dma((n_split,)),
        ],
        compiler_params=pltpu.CompilerParams(
            collective_id=0, has_side_effects=True, vmem_limit_bytes=48 * 1024 * 1024
        ),
        name="hartree",
    )(miller, form_factors, fractional, multipoles, point_owner, offsets)


def solution(mesh):
    placed = (
        P(None, "gsplit"),
        P(None, "gsplit"),
        P(None, "atoms"),
        P(None, None, "atoms"),
        P(("atoms", "gsplit")),
        P(None, ("atoms", "gsplit")),
    )
    return jax.shard_map(
        functools.partial(shards, mesh.shape["atoms"], mesh.shape["gsplit"]),
        mesh=mesh,
        in_specs=placed,
        out_specs=(P(None, ("atoms", "gsplit")), P(None, None, ("atoms", "gsplit"))),
        check_vma=False,
    )
```

```python
import functools

import jax
import jax.numpy as jnp
from jax import lax
from jax.experimental import pallas as pl
from jax.experimental.pallas import tpu as pltpu
from jax.sharding import PartitionSpec as P

damping = 1.0 / 400.0
MESH = pl.DeviceIdType.MESH
f32 = jnp.float32
bf16 = jnp.bfloat16

SIN_COEFS = (4.442879567546084, -7.30781668449178, 3.5977741780871235, -0.7911993921609659)
COS_COEFS = (
    1.4142134962552286,
    -6.978850948563789,
    5.73946037690675,
    -1.8835579059841712,
    0.3106880275217573,
)


def poly(coefs, x):
    total = coefs[-1]
    for coef in coefs[-2::-1]:
        total = total * x + coef
    return total


def cos_sin(turns):
    r = turns - jnp.round(turns)
    square = r * r
    half_sin = r * poly(SIN_COEFS, square)
    half_cos = poly(COS_COEFS, square)
    return (1.0 - half_sin * half_sin).astype(bf16), (half_sin * half_cos).astype(bf16)


def three_parts(x):
    first = x.astype(bf16).astype(f32)
    rest = x - first
    second = rest.astype(bf16).astype(f32)
    third = rest - second
    return jnp.concatenate([first, second, third, jnp.zeros_like(x)], axis=0)


def row_signs(comps, rows):
    ids = lax.broadcasted_iota(jnp.int32, (rows, 1), 0)
    degree = jnp.zeros_like(ids)
    for step in range(1, 16):
        if step * step < comps:
            degree = degree + (ids >= step * step).astype(jnp.int32)
    quarter = lax.rem(degree, 4)
    quarter = jnp.where(ids == comps, 0, quarter)
    even = (quarter == 0) | (quarter == 2)
    sign = jnp.where((quarter == 0) | (quarter == 3), 1.0, -1.0).astype(f32)
    return even, sign


def kernel(
    n_atoms, n_split, chunk,
    miller_hbm, form_hbm, frac_hbm, mult_hbm, owner_hbm, offs_hbm,
    grid_out, mom_out,
    miller_ref, form_ref, frac_ref, mult_ref, owner_ref, offs_ref,
    vec8, fx, tcos, tsin, partial, from_core, acc, chip_out, chip_in, total,
    place_buf, send_buf, recv_buf,
    load_sems, core_send, core_recv, chip_send, chip_recv, back_send, back_recv,
    place_send, place_recv, out_send, out_recv,
):
    me = lax.axis_index("atoms")
    mine = lax.axis_index("gsplit")
    loads = [
        pltpu.make_async_copy(src, dst, load_sems.at[k])
        for k, (src, dst) in enumerate((
            (owner_hbm, owner_ref), (offs_hbm, offs_ref), (frac_hbm, frac_ref),
            (mult_hbm, mult_ref), (miller_hbm, miller_ref), (form_hbm, form_ref),
        ))
    ]
    for load in loads:
        load.start()
    comps, dens, atoms = mult_ref.shape
    rows = fx.shape[0]
    width = partial.shape[3]
    steps = width // chunk
    points = n_split * owner_ref.shape[0]
    own_points = owner_ref.shape[0]
    chips = n_atoms // 2
    core = lax.rem(me, 2)
    other = 1 - core

    def flipped(mask):
        there = me
        for bit in range(mask.bit_length()):
            if mask >> bit & 1:
                there = there + (1 - 2 * lax.rem(lax.div(me, 2**bit), 2)) * 2**bit
        return there

    greeted = [1] + [2 * away for away in range(1, chips)]

    barrier = pltpu.get_barrier_semaphore()
    for mask in greeted:
        pl.semaphore_signal(barrier, inc=1, device_id={"atoms": flipped(mask)}, device_id_type=MESH)
    for away in range(1, n_split):
        pl.semaphore_signal(
            barrier, inc=1, device_id={"gsplit": lax.rem(mine + away, n_split)}, device_id_type=MESH
        )

    even, sign = row_signs(comps, rows)

    tail = (comps // 8) * 8
    tail_ids = lax.broadcasted_iota(jnp.int32, (rows - tail, fx.shape[1]), 0)
    fx[tail:rows, :] = jnp.where(tail_ids == comps - tail, 1.0, 0.0).astype(f32)
    vec8[...] = jnp.zeros_like(vec8)
    for load in loads[:4]:
        load.wait()

    frac8 = jnp.concatenate([frac_ref[...], jnp.zeros((5, atoms), f32)], axis=0)
    frac_parts = three_parts(frac8)
    atom_ids = lax.broadcasted_iota(jnp.int32, (atoms, own_points), 0)
    onehot = (atom_ids == owner_ref[...].reshape(1, own_points)).astype(f32).astype(bf16)
    picked = jnp.dot(frac_parts.astype(bf16), onehot, preferred_element_type=f32)
    place = (picked[0:8] + picked[8:16]) + picked[16:24]
    place_buf[mine, :, :] = jnp.zeros(place_buf.shape[1:], f32)
    place_buf[mine, :, 0:own_points] = place
    place_buf[mine, 0:3, 0:own_points] = place[0:3] + offs_ref[...]

    def widened(block):
        pad = jnp.zeros((block.shape[0], 128 - block.shape[1]), f32)
        return jnp.concatenate([block, pad], axis=1).T if pad.shape[1] else block.T

    atom_parts = widened(frac_parts)[0:atoms].astype(bf16)

    multipoles = mult_ref[...].astype(f32)
    groups = []
    for part in range(2):
        for d in range(dens):
            m = jnp.concatenate(
                [multipoles[:, d, :], jnp.zeros((rows - comps, atoms), f32)], axis=0
            )
            if part == 0:
                with_cos, with_sin = jnp.where(even, m, 0.0), jnp.where(even, 0.0, m)
            else:
                with_cos, with_sin = jnp.where(even, 0.0, m), jnp.where(even, -m, 0.0)
            groups.append(jnp.concatenate([with_cos, with_sin], axis=1))
    against = jnp.concatenate(groups, axis=0).astype(bf16)

    def vectors(half, quarter, i):
        start = pl.multiple_of(half * 2 * width + quarter * width + i * chunk, 128)
        return pl.ds(start, chunk)

    def turns(parts, where):
        v = vec8[:, where]
        wide = jnp.concatenate([v, v, v, jnp.zeros_like(v)], axis=0).astype(bf16)
        return jnp.dot(parts, wide, preferred_element_type=f32)

    def within(quarter, i):
        return pl.ds(pl.multiple_of(quarter * width + i * chunk, 128), chunk)

    def structure(half, quarter):
        def body(i, carry):
            where = vectors(half, quarter, i)
            inside = within(quarter, i)
            c, s = cos_sin(turns(atom_parts, where))
            tcos[half, 0:atoms, inside] = c
            tsin[half, 0:atoms, inside] = s
            both = jnp.concatenate([c, s], axis=0)
            along = jnp.dot(against, both, preferred_element_type=f32)
            fx[0:comps, where] = form_ref[:, where].astype(f32) * sign[0:comps]
            f = fx[:, where]
            sums = [
                jnp.sum(f * along[k * rows : (k + 1) * rows], axis=0, keepdims=True)
                for k in range(2 * dens)
            ]
            lanes = pl.ds(pl.multiple_of(i * chunk, 128), chunk)
            partial[half, quarter, :, lanes] = jnp.concatenate(sums, axis=0)
            return carry

        lax.fori_loop(0, steps, body, 0, unroll=steps)

    loads[4].wait()
    vec8[0:3, :] = miller_ref[...].astype(f32)
    loads[5].wait()

    structure(other, 0)

    pl.semaphore_wait(barrier, len(greeted) + n_split - 1)

    place_copies = []
    for away in range(1, n_split):
        copy = pltpu.make_async_remote_copy(
            src_ref=place_buf.at[mine],
            dst_ref=place_buf.at[mine],
            send_sem=place_send.at[away],
            recv_sem=place_recv.at[away],
            device_id={"gsplit": lax.rem(mine + away, n_split)},
            device_id_type=MESH,
        )
        copy.start()
        place_copies.append(copy)

    def to_core(quarter):
        copy = pltpu.make_async_remote_copy(
            src_ref=partial.at[other, quarter],
            dst_ref=from_core.at[quarter],
            send_sem=core_send.at[quarter],
            recv_sem=core_recv.at[quarter],
            device_id={"atoms": flipped(1)},
            device_id_type=MESH,
        )
        copy.start()
        return copy

    def to_chips(quarter, arriving):
        arriving.wait()
        summed = partial[core, quarter] + from_core[quarter]
        acc[quarter] = summed
        chip_out[quarter] = summed.astype(bf16)
        copies = []
        for away in range(1, chips):
            copy = pltpu.make_async_remote_copy(
                src_ref=chip_out.at[quarter],
                dst_ref=chip_in.at[away, quarter],
                send_sem=chip_send.at[away, quarter],
                recv_sem=chip_recv.at[away, quarter],
                device_id={"atoms": flipped(2 * away)},
                device_id_type=MESH,
            )
            copy.start()
            copies.append(copy)
        return copies

    def back(quarter, copies):
        summed = acc[quarter]
        for away, copy in enumerate(copies, 1):
            copy.wait()
            summed = summed + chip_in[away, quarter].astype(f32)
        total[core, quarter] = summed
        copy = pltpu.make_async_remote_copy(
            src_ref=total.at[core, quarter],
            dst_ref=total.at[core, quarter],
            send_sem=back_send.at[quarter],
            recv_sem=back_recv.at[quarter],
            device_id={"atoms": flipped(1)},
            device_id_type=MESH,
        )
        copy.start()
        return copy

    first = to_core(0)
    structure(core, 0)
    structure(other, 1)
    second = to_core(1)
    first = to_chips(0, first)
    structure(core, 1)
    second = to_chips(1, second)

    for copy in place_copies:
        copy.wait()
    pieces = [three_parts(place_buf[k, :, 0:own_points]) for k in range(n_split)]
    point_parts = widened(jnp.concatenate(pieces, axis=1))[0:points].astype(bf16)

    def point_tables(half, quarter):
        def body(i, carry):
            inside = within(quarter, i)
            c, s = cos_sin(turns(point_parts, vectors(half, quarter, i)))
            tcos[half, atoms : atoms + points, inside] = c
            tsin[half, atoms : atoms + points, inside] = s
            return carry

        lax.fori_loop(0, steps, body, 0)

    point_tables(0, 0)
    point_tables(0, 1)
    first = back(0, first)
    point_tables(1, 0)
    point_tables(1, 1)
    second = back(1, second)

    def moments(half):
        result = None
        for quarter in range(2):
            start = pl.multiple_of(half * 2 * width + quarter * width, 128)
            where = pl.ds(start, width)
            v = vec8[:, where]
            q = jnp.sum(v * v, axis=0, keepdims=True)
            pot = (jnp.exp(-damping * q) / q) * total[half, quarter]
            f = fx[:, where]
            lanes = slice(quarter * width, (quarter + 1) * width)
            with_cos, with_sin = [], []
            for d in range(dens):
                re, im = pot[d : d + 1], pot[dens + d : dens + d + 1]
                with_cos.append(f * jnp.where(even, re, im))
                with_sin.append(f * jnp.where(even, -im, re))
            for table, weights in ((tcos, with_cos), (tsin, with_sin)):
                term = lax.dot_general(
                    table[half, :, lanes],
                    jnp.concatenate(weights, axis=0).astype(bf16),
                    (((1,), (1,)), ((), ())),
                    preferred_element_type=f32,
                )
                result = term if result is None else result + term
        return result

    own = moments(core)
    first.wait()
    second.wait()
    local = own + moments(other)

    pad = jnp.zeros((local.shape[0], 128 - local.shape[1]), f32)
    local = jnp.concatenate([local, pad], axis=1)
    grid_rows = local[atoms : atoms + points].T
    share = atoms // n_split
    for k in range(n_split):
        send_buf[k, 0:share, :] = local[k * share : (k + 1) * share]
        send_buf[k, share:, :] = jnp.zeros((8, 128), f32)
        for d in range(dens):
            row = d * rows + comps
            send_buf[k, share + d : share + d + 1, 0:own_points] = grid_rows[
                row : row + 1, k * own_points : (k + 1) * own_points
            ]
    out_copies = []
    for away in range(1, n_split):
        there = lax.rem(mine + away, n_split)
        copy = pltpu.make_async_remote_copy(
            src_ref=send_buf.at[there, 0 : share + dens],
            dst_ref=recv_buf.at[away, 0 : share + dens],
            send_sem=out_send.at[away],
            recv_sem=out_recv.at[away],
            device_id={"gsplit": there},
            device_id_type=MESH,
        )
        copy.start()
        out_copies.append(copy)
    result = send_buf[mine, 0 : share + dens]
    for away, copy in enumerate(out_copies, 1):
        copy.wait()
        result = result + recv_buf[away, 0 : share + dens]
    grid_out[...] = result[share : share + dens, 0:own_points]
    for d in range(dens):
        mom_out[d] = result[0:share, d * rows : d * rows + comps]


def shards(n_atoms, n_split, miller, form_factors, fractional, multipoles, point_owner, offsets):
    dens, comps, atoms = multipoles.shape
    vectors = miller.shape[1]
    width = vectors // 4
    chunk = max(c for c in (128, 256, 384) if width % c == 0)
    rows = (comps + 1 + 7) // 8 * 8
    own_points = point_owner.shape[0]
    table_rows = atoms + n_split * own_points
    chips = n_atoms // 2
    share = atoms // n_split
    vmem = pl.BlockSpec(memory_space=pltpu.VMEM)
    dma = pltpu.SemaphoreType.DMA
    hbm = pl.BlockSpec(memory_space=pltpu.HBM)
    grid, moments = pl.pallas_call(
        functools.partial(kernel, n_atoms, n_split, chunk),
        out_shape=(
            jax.ShapeDtypeStruct((dens, own_points), f32),
            jax.ShapeDtypeStruct((dens, share, comps), f32),
        ),
        in_specs=[hbm] * 6,
        out_specs=(vmem, vmem),
        scratch_shapes=[
            pltpu.VMEM(miller.shape, miller.dtype),
            pltpu.VMEM(form_factors.shape, form_factors.dtype),
            pltpu.VMEM(fractional.shape, fractional.dtype),
            pltpu.VMEM((comps, dens, atoms), multipoles.dtype),
            pltpu.VMEM(point_owner.shape, point_owner.dtype),
            pltpu.VMEM(offsets.shape, offsets.dtype),
            pltpu.VMEM((8, vectors), f32),
            pltpu.VMEM((rows, vectors), f32),
            pltpu.VMEM((2, table_rows, 2 * width), bf16),
            pltpu.VMEM((2, table_rows, 2 * width), bf16),
            pltpu.VMEM((2, 2, 2 * dens, width), f32),
            pltpu.VMEM((2, 2 * dens, width), f32),
            pltpu.VMEM((2, 2 * dens, width), f32),
            pltpu.VMEM((2, 2 * dens, width), bf16),
            pltpu.VMEM((chips, 2, 2 * dens, width), bf16),
            pltpu.VMEM((2, 2, 2 * dens, width), f32),
            pltpu.VMEM((n_split, 8, 128), f32),
            pltpu.VMEM((n_split, share + 8, 128), f32),
            pltpu.VMEM((n_split, share + 8, 128), f32),
            dma((6,)),
            dma((2,)),
            dma((2,)),
            dma((chips, 2)),
            dma((chips, 2)),
            dma((2,)),
            dma((2,)),
            dma((n_split,)),
            dma((n_split,)),
            dma((n_split,)),
            dma((n_split,)),
        ],
        compiler_params=pltpu.CompilerParams(
            collective_id=0, has_side_effects=True, vmem_limit_bytes=67_043_328
        ),
        name="hartree",
    )(
        miller,
        form_factors,
        fractional,
        jnp.transpose(multipoles, (1, 0, 2)),
        point_owner,
        offsets,
    )
    return grid, jnp.transpose(moments, (0, 2, 1))


def solution(mesh):
    placed = (
        P(None, "gsplit"),
        P(None, "gsplit"),
        P(None, "atoms"),
        P(None, None, "atoms"),
        P(("atoms", "gsplit")),
        P(None, ("atoms", "gsplit")),
    )
    return jax.shard_map(
        functools.partial(shards, mesh.shape["atoms"], mesh.shape["gsplit"]),
        mesh=mesh,
        in_specs=placed,
        out_specs=(P(None, ("atoms", "gsplit")), P(None, None, ("atoms", "gsplit"))),
        check_vma=False,
    )
```

```python
import functools

import jax
import jax.numpy as jnp
from jax import lax
from jax.experimental import pallas as pl
from jax.experimental.pallas import tpu as pltpu
from jax.sharding import PartitionSpec as P

damping = 1.0 / 400.0
MESH = pl.DeviceIdType.MESH
f32 = jnp.float32
bf16 = jnp.bfloat16

SIN_COEFS = (4.442879567546084, -7.30781668449178, 3.5977741780871235, -0.7911993921609659)
COS_COEFS = (
    1.4142134962552286,
    -6.978850948563789,
    5.73946037690675,
    -1.8835579059841712,
    0.3106880275217573,
)


def poly(coefs, x):
    total = coefs[-1]
    for coef in coefs[-2::-1]:
        total = total * x + coef
    return total


def cos_sin(turns):
    r = turns - jnp.round(turns)
    square = r * r
    half_sin = r * poly(SIN_COEFS, square)
    half_cos = poly(COS_COEFS, square)
    return (1.0 - half_sin * half_sin).astype(bf16), (half_sin * half_cos).astype(bf16)


def three_parts(x):
    first = x.astype(bf16).astype(f32)
    rest = x - first
    second = rest.astype(bf16).astype(f32)
    third = rest - second
    return jnp.concatenate([first, second, third, jnp.zeros_like(x)], axis=0)


def row_signs(comps, rows):
    ids = lax.broadcasted_iota(jnp.int32, (rows, 1), 0)
    degree = jnp.zeros_like(ids)
    for step in range(1, 16):
        if step * step < comps:
            degree = degree + (ids >= step * step).astype(jnp.int32)
    quarter = lax.rem(degree, 4)
    quarter = jnp.where(ids == comps, 0, quarter)
    even = (quarter == 0) | (quarter == 2)
    sign = jnp.where((quarter == 0) | (quarter == 3), 1.0, -1.0).astype(f32)
    return even, sign


def kernel(
    n_atoms, n_split, chunk,
    miller_hbm, form_hbm, frac_hbm, mult_hbm, owner_hbm, offs_hbm,
    grid_out, mom_out,
    miller_ref, form_ref, frac_ref, mult_ref, owner_ref, offs_ref,
    vec8, fx, tcos, tsin, partial, from_core, acc, chip_out, chip_in, total,
    place_buf, send_buf, recv_buf,
    load_sems, core_send, core_recv, chip_send, chip_recv, back_send, back_recv,
    place_send, place_recv, out_send, out_recv,
):
    me = lax.axis_index("atoms")
    mine = lax.axis_index("gsplit")
    loads = [
        pltpu.make_async_copy(src, dst, load_sems.at[k])
        for k, (src, dst) in enumerate((
            (owner_hbm, owner_ref), (offs_hbm, offs_ref), (frac_hbm, frac_ref),
            (mult_hbm, mult_ref), (miller_hbm, miller_ref), (form_hbm, form_ref),
        ))
    ]
    for load in loads:
        load.start()
    comps, dens, atoms = mult_ref.shape
    rows = fx.shape[0]
    width = partial.shape[3]
    steps = width // chunk
    points = n_split * owner_ref.shape[0]
    own_points = owner_ref.shape[0]
    chips = n_atoms // 2
    core = lax.rem(me, 2)
    other = 1 - core

    def flipped(mask):
        there = me
        for bit in range(mask.bit_length()):
            if mask >> bit & 1:
                there = there + (1 - 2 * lax.rem(lax.div(me, 2**bit), 2)) * 2**bit
        return there

    greeted = [1] + [2 * away for away in range(1, chips)]

    barrier = pltpu.get_barrier_semaphore()
    for mask in greeted:
        pl.semaphore_signal(barrier, inc=1, device_id={"atoms": flipped(mask)}, device_id_type=MESH)
    for away in range(1, n_split):
        pl.semaphore_signal(
            barrier, inc=1, device_id={"gsplit": lax.rem(mine + away, n_split)}, device_id_type=MESH
        )

    even, sign = row_signs(comps, rows)

    tail = (comps // 8) * 8
    tail_ids = lax.broadcasted_iota(jnp.int32, (rows - tail, fx.shape[1]), 0)
    fx[tail:rows, :] = jnp.where(tail_ids == comps - tail, 1.0, 0.0).astype(f32)
    vec8[...] = jnp.zeros_like(vec8)
    for load in loads[:4]:
        load.wait()

    frac8 = jnp.concatenate([frac_ref[...], jnp.zeros((5, atoms), f32)], axis=0)
    frac_parts = three_parts(frac8)
    atom_ids = lax.broadcasted_iota(jnp.int32, (atoms, own_points), 0)
    onehot = (atom_ids == owner_ref[...].reshape(1, own_points)).astype(f32).astype(bf16)
    picked = jnp.dot(frac_parts.astype(bf16), onehot, preferred_element_type=f32)
    place = (picked[0:8] + picked[8:16]) + picked[16:24]
    place_buf[mine, :, :] = jnp.zeros(place_buf.shape[1:], f32)
    place_buf[mine, :, 0:own_points] = place
    place_buf[mine, 0:3, 0:own_points] = place[0:3] + offs_ref[...]

    def widened(block):
        pad = jnp.zeros((block.shape[0], 128 - block.shape[1]), f32)
        return jnp.concatenate([block, pad], axis=1).T if pad.shape[1] else block.T

    atom_parts = widened(frac_parts)[0:atoms].astype(bf16)

    multipoles = mult_ref[...].astype(f32)
    groups = []
    for part in range(2):
        for d in range(dens):
            m = jnp.concatenate(
                [multipoles[:, d, :], jnp.zeros((rows - comps, atoms), f32)], axis=0
            )
            if part == 0:
                with_cos, with_sin = jnp.where(even, m, 0.0), jnp.where(even, 0.0, m)
            else:
                with_cos, with_sin = jnp.where(even, 0.0, m), jnp.where(even, -m, 0.0)
            groups.append(jnp.concatenate([with_cos, with_sin], axis=1))
    against = jnp.concatenate(groups, axis=0).astype(bf16)

    def vectors(half, quarter, i):
        start = pl.multiple_of(half * 2 * width + quarter * width + i * chunk, 128)
        return pl.ds(start, chunk)

    def turns(parts, where):
        v = vec8[:, where]
        wide = jnp.concatenate([v, v, v, jnp.zeros_like(v)], axis=0).astype(bf16)
        return jnp.dot(parts, wide, preferred_element_type=f32)

    def within(quarter, i):
        return pl.ds(pl.multiple_of(quarter * width + i * chunk, 128), chunk)

    def structure(half, quarter):
        def body(i, carry):
            where = vectors(half, quarter, i)
            inside = within(quarter, i)
            c, s = cos_sin(turns(atom_parts, where))
            tcos[half, 0:atoms, inside] = c
            tsin[half, 0:atoms, inside] = s
            both = jnp.concatenate([c, s], axis=0)
            along = jnp.dot(against, both, preferred_element_type=f32)
            fx[0:comps, where] = form_ref[:, where].astype(f32) * sign[0:comps]
            f = fx[:, where]
            sums = [
                jnp.sum(f * along[k * rows : (k + 1) * rows], axis=0, keepdims=True)
                for k in range(2 * dens)
            ]
            lanes = pl.ds(pl.multiple_of(i * chunk, 128), chunk)
            partial[half, quarter, :, lanes] = jnp.concatenate(sums, axis=0)
            return carry

        lax.fori_loop(0, steps, body, 0, unroll=steps)

    loads[4].wait()
    vec8[0:3, :] = miller_ref[...].astype(f32)
    loads[5].wait()

    structure(other, 0)

    pl.semaphore_wait(barrier, len(greeted) + n_split - 1)

    place_copies = []
    for away in range(1, n_split):
        copy = pltpu.make_async_remote_copy(
            src_ref=place_buf.at[mine],
            dst_ref=place_buf.at[mine],
            send_sem=place_send.at[away],
            recv_sem=place_recv.at[away],
            device_id={"gsplit": lax.rem(mine + away, n_split)},
            device_id_type=MESH,
        )
        copy.start()
        place_copies.append(copy)

    def to_core(quarter):
        copy = pltpu.make_async_remote_copy(
            src_ref=partial.at[other, quarter],
            dst_ref=from_core.at[quarter],
            send_sem=core_send.at[quarter],
            recv_sem=core_recv.at[quarter],
            device_id={"atoms": flipped(1)},
            device_id_type=MESH,
        )
        copy.start()
        return copy

    def to_chips(quarter, arriving):
        arriving.wait()
        summed = partial[core, quarter] + from_core[quarter]
        acc[quarter] = summed
        chip_out[quarter] = summed
        copies = []
        for away in range(1, chips):
            copy = pltpu.make_async_remote_copy(
                src_ref=chip_out.at[quarter],
                dst_ref=chip_in.at[away, quarter],
                send_sem=chip_send.at[away, quarter],
                recv_sem=chip_recv.at[away, quarter],
                device_id={"atoms": flipped(2 * away)},
                device_id_type=MESH,
            )
            copy.start()
            copies.append(copy)
        return copies

    def back(quarter, copies):
        summed = acc[quarter]
        for away, copy in enumerate(copies, 1):
            copy.wait()
            summed = summed + chip_in[away, quarter]
        total[core, quarter] = summed
        copy = pltpu.make_async_remote_copy(
            src_ref=total.at[core, quarter],
            dst_ref=total.at[core, quarter],
            send_sem=back_send.at[quarter],
            recv_sem=back_recv.at[quarter],
            device_id={"atoms": flipped(1)},
            device_id_type=MESH,
        )
        copy.start()
        return copy

    first = to_core(0)
    structure(core, 0)
    structure(other, 1)
    second = to_core(1)
    first = to_chips(0, first)
    structure(core, 1)
    second = to_chips(1, second)

    for copy in place_copies:
        copy.wait()
    pieces = [three_parts(place_buf[k, :, 0:own_points]) for k in range(n_split)]
    point_parts = widened(jnp.concatenate(pieces, axis=1))[0:points].astype(bf16)

    def point_tables(half, quarter):
        def body(i, carry):
            inside = within(quarter, i)
            c, s = cos_sin(turns(point_parts, vectors(half, quarter, i)))
            tcos[half, atoms : atoms + points, inside] = c
            tsin[half, atoms : atoms + points, inside] = s
            return carry

        lax.fori_loop(0, steps, body, 0)

    point_tables(0, 0)
    point_tables(0, 1)
    first = back(0, first)
    point_tables(1, 0)
    point_tables(1, 1)
    second = back(1, second)

    def moments(half):
        result = None
        for quarter in range(2):
            start = pl.multiple_of(half * 2 * width + quarter * width, 128)
            where = pl.ds(start, width)
            v = vec8[:, where]
            q = jnp.sum(v * v, axis=0, keepdims=True)
            pot = (jnp.exp(-damping * q) / q) * total[half, quarter]
            f = fx[:, where]
            lanes = slice(quarter * width, (quarter + 1) * width)
            with_cos, with_sin = [], []
            for d in range(dens):
                re, im = pot[d : d + 1], pot[dens + d : dens + d + 1]
                with_cos.append(f * jnp.where(even, re, im))
                with_sin.append(f * jnp.where(even, -im, re))
            for table, weights in ((tcos, with_cos), (tsin, with_sin)):
                term = lax.dot_general(
                    table[half, :, lanes],
                    jnp.concatenate(weights, axis=0).astype(bf16),
                    (((1,), (1,)), ((), ())),
                    preferred_element_type=f32,
                )
                result = term if result is None else result + term
        return result

    own = moments(core)
    first.wait()
    second.wait()
    local = own + moments(other)

    pad = jnp.zeros((local.shape[0], 128 - local.shape[1]), f32)
    local = jnp.concatenate([local, pad], axis=1)
    grid_rows = local[atoms : atoms + points].T
    share = atoms // n_split
    for k in range(n_split):
        send_buf[k, 0:share, :] = local[k * share : (k + 1) * share]
        send_buf[k, share:, :] = jnp.zeros((8, 128), f32)
        for d in range(dens):
            row = d * rows + comps
            send_buf[k, share + d : share + d + 1, 0:own_points] = grid_rows[
                row : row + 1, k * own_points : (k + 1) * own_points
            ]
    out_copies = []
    for away in range(1, n_split):
        there = lax.rem(mine + away, n_split)
        copy = pltpu.make_async_remote_copy(
            src_ref=send_buf.at[there, 0 : share + dens],
            dst_ref=recv_buf.at[away, 0 : share + dens],
            send_sem=out_send.at[away],
            recv_sem=out_recv.at[away],
            device_id={"gsplit": there},
            device_id_type=MESH,
        )
        copy.start()
        out_copies.append(copy)
    result = send_buf[mine, 0 : share + dens]
    for away, copy in enumerate(out_copies, 1):
        copy.wait()
        result = result + recv_buf[away, 0 : share + dens]
    grid_out[...] = result[share : share + dens, 0:own_points]
    for d in range(dens):
        mom_out[d] = result[0:share, d * rows : d * rows + comps]


def shards(n_atoms, n_split, miller, form_factors, fractional, multipoles, point_owner, offsets):
    dens, comps, atoms = multipoles.shape
    vectors = miller.shape[1]
    width = vectors // 4
    chunk = max(c for c in (128, 256, 384) if width % c == 0)
    rows = (comps + 1 + 7) // 8 * 8
    own_points = point_owner.shape[0]
    table_rows = atoms + n_split * own_points
    chips = n_atoms // 2
    share = atoms // n_split
    vmem = pl.BlockSpec(memory_space=pltpu.VMEM)
    dma = pltpu.SemaphoreType.DMA
    hbm = pl.BlockSpec(memory_space=pltpu.HBM)
    grid, moments = pl.pallas_call(
        functools.partial(kernel, n_atoms, n_split, chunk),
        out_shape=(
            pltpu.VMEM((dens, own_points), f32),
            pltpu.VMEM((dens, share, comps), f32),
        ),
        in_specs=[hbm] * 6,
        out_specs=(vmem, vmem),
        scratch_shapes=[
            pltpu.VMEM(miller.shape, miller.dtype),
            pltpu.VMEM(form_factors.shape, form_factors.dtype),
            pltpu.VMEM(fractional.shape, fractional.dtype),
            pltpu.VMEM((comps, dens, atoms), multipoles.dtype),
            pltpu.VMEM(point_owner.shape, point_owner.dtype),
            pltpu.VMEM(offsets.shape, offsets.dtype),
            pltpu.VMEM((8, vectors), f32),
            pltpu.VMEM((rows, vectors), f32),
            pltpu.VMEM((2, table_rows, 2 * width), bf16),
            pltpu.VMEM((2, table_rows, 2 * width), bf16),
            pltpu.VMEM((2, 2, 2 * dens, width), f32),
            pltpu.VMEM((2, 2 * dens, width), f32),
            pltpu.VMEM((2, 2 * dens, width), f32),
            pltpu.VMEM((2, 2 * dens, width), f32),
            pltpu.VMEM((chips, 2, 2 * dens, width), f32),
            pltpu.VMEM((2, 2, 2 * dens, width), f32),
            pltpu.VMEM((n_split, 8, 128), f32),
            pltpu.VMEM((n_split, share + 8, 128), f32),
            pltpu.VMEM((n_split, share + 8, 128), f32),
            dma((6,)),
            dma((2,)),
            dma((2,)),
            dma((chips, 2)),
            dma((chips, 2)),
            dma((2,)),
            dma((2,)),
            dma((n_split,)),
            dma((n_split,)),
            dma((n_split,)),
            dma((n_split,)),
        ],
        compiler_params=pltpu.CompilerParams(
            collective_id=0, has_side_effects=True, vmem_limit_bytes=60_000_000
        ),
        name="hartree",
    )(
        miller,
        form_factors,
        fractional,
        jnp.transpose(multipoles, (1, 0, 2)),
        point_owner,
        offsets,
    )
    return grid, jnp.transpose(moments, (0, 2, 1))


def solution(mesh):
    placed = (
        P(None, "gsplit"),
        P(None, "gsplit"),
        P(None, "atoms"),
        P(None, None, "atoms"),
        P(("atoms", "gsplit")),
        P(None, ("atoms", "gsplit")),
    )
    return jax.shard_map(
        functools.partial(shards, mesh.shape["atoms"], mesh.shape["gsplit"]),
        mesh=mesh,
        in_specs=placed,
        out_specs=(P(None, ("atoms", "gsplit")), P(None, None, ("atoms", "gsplit"))),
        check_vma=False,
    )
```
